32 devices in a mesh: dp: 8 (over z, y), mp: 4 (over x, core).
Axes of the slice: x: 2, y: 2, z: 4, core: 2. Of those that a mesh axis runs over, the one named last changes fastest.
Arguments:
- hidden_in: bfloat16 [16384, 1536], P(('dp', 'mp')), may hold values from -6 to 6
- text_states: bfloat16 [10240, 4096], P('dp'), may hold values from -6 to 6
- modulation: float32 [8, 5, 6144], P('dp'), may hold values from -3 to 3
- image_lengths: int32 [8, 5], P('dp'), may hold values from 1 to 1088, as said below
- text_lengths: int32 [8, 5], P('dp'), may hold values from 32 to 256
- positions: int32 [2, 16384], P(None, 'dp'), may hold values from 0 to 64, as said below
- w_query: bfloat16 [1536, 1536], P(None, 'mp'), may hold values from -0.15625 to 0.15625
- w_key: bfloat16 [1536, 1536], P(None, 'mp'), may hold values from -0.15625 to 0.15625
- w_value: bfloat16 [1536, 1536], P(None, 'mp'), may hold values from -0.15625 to 0.15625
- w_out: bfloat16 [1536, 1536], P('mp'), may hold values from -0.625 to 0.625
- w_text_key: bfloat16 [4096, 1536], P(None, 'mp'), may hold values from -0.09375 to 0.09375
- w_text_value: bfloat16 [4096, 1536], P(None, 'mp'), may hold values from -0.09375 to 0.09375
- w_gate: bfloat16 [1536, 4096], P(None, 'mp'), may hold values from -0.15625 to 0.15625
- w_up: bfloat16 [1536, 4096], P(None, 'mp'), may hold values from -0.15625 to 0.15625
- w_down: bfloat16 [4096, 1536], P('mp'), may hold values from -0.09375 to 0.09375
- attention_gain: float32 [1536], replicated, may hold values from 0.5 to 1.5
- feedforward_gain: float32 [1536], replicated, may hold values from 0.5 to 1.5
- head_gates: float32 [24], replicated, may hold values from 0.3 to 1.2
- out_cotangent: bfloat16 [16384, 1536], P(('dp', 'mp')), may hold values from -6 to 6
Outputs:
- block_out: bfloat16 [16384, 1536], P(('dp', 'mp'))
- input_grad: bfloat16 [16384, 1536], P(('dp', 'mp'))
- modulation_grad: float32 [8, 5, 6144], P('dp')
- grad_w_query: float32 [1536, 1536], P('dp', 'mp')
- grad_w_key: float32 [1536, 1536], P('dp', 'mp')
- grad_w_value: float32 [1536, 1536], P('dp', 'mp')
- grad_w_out: float32 [1536, 1536], P('mp', 'dp')
- grad_w_text_key: float32 [4096, 1536], P('dp', 'mp')
- grad_w_text_value: float32 [4096, 1536], P('dp', 'mp')
- grad_w_gate: float32 [1536, 4096], P('dp', 'mp')
- grad_w_up: float32 [1536, 4096], P('dp', 'mp')
- grad_w_down: float32 [4096, 1536], P('mp', 'dp')
- grad_attention_gain: float32 [1536], replicated
- grad_feedforward_gain: float32 [1536], replicated
- grad_head_gates: float32 [24], replicated
The draws below stay inside these ranges and needn't reach their ends.
Inputs may be any that keep to these rules, and one draw needn't show every extreme that they name: `image_lengths`: each row holds the 5 segment lengths of one pack, summing to 2048. The first 4 are images in some order: one of r rows and c columns of patches with r c = 32^2 and three with r c = 16^2, each with r in (side/2, side, 2 side) and one nextline token a row, so r (c + 1) tokens; the last segment is a filler. `positions`: row 0 holds each token's row in its segment's grid, row 1 its column; a nextline token takes column c; the filler continues a grid of 32 columns.
All inputs are finite; a program needn't handle non-finite values.
Results may differ from the reference program's by a relative error of at most 0.018.
Values may be sent and summed in bfloat16 or wider, within the bound.
A program may use at most 576 MiB of HBM per device.

```python
import jax
import jax.numpy as jnp
from jax import lax

D = 1536
H = 24
HD = 64
FF = 4096
TD = 4096
TXT = 256
SIDE = 32
IMGS = 5
SEQ = 2048
TOKENS = 16384
TEXT_ROWS = 10240
N_DP = 8


def segment_layout(key):
    base_key = jax.random.fold_in(key, 913)
    aspect_key = jax.random.fold_in(base_key, 1)
    order_key = jax.random.fold_in(base_key, 2)
    aspect = jax.random.randint(aspect_key, (N_DP, 4), 0, 3).astype(jnp.int32)
    aspect = aspect.at[0, 0].set(2).at[1, 0].set(1)
    sides = jnp.array([SIDE, SIDE // 2, SIDE // 2, SIDE // 2], jnp.int32)[None, :]
    grid_rows = jnp.where(aspect == 0, sides, jnp.where(aspect == 1, sides // 2, 2 * sides))
    grid_cols = jnp.where(aspect == 0, sides, jnp.where(aspect == 1, 2 * sides, sides // 2))
    order = jax.vmap(lambda k: jax.random.permutation(k, 4))(jax.random.split(order_key, N_DP)).astype(jnp.int32)
    grid_rows = jnp.take_along_axis(grid_rows, order, 1)
    grid_cols = jnp.take_along_axis(grid_cols, order, 1)
    image_sizes = grid_rows * (grid_cols + 1)
    filler = SEQ - jnp.sum(image_sizes, 1, keepdims=True)
    lengths = jnp.concatenate([image_sizes, filler], 1).astype(jnp.int32)
    columns = jnp.concatenate([grid_cols, jnp.full((N_DP, 1), SIDE, jnp.int32)], 1)
    return (lengths, columns)


def draw_image_lengths(key, part):
    return segment_layout(key)[0]


def draw_positions(key, part):
    lengths, columns = segment_layout(key)
    ends = jnp.cumsum(lengths, 1).astype(jnp.int32)
    starts = ends - lengths
    token_ids = jnp.arange(SEQ, dtype=jnp.int32)
    segment = jnp.sum((token_ids[None, :, None] >= ends[:, None, :]).astype(jnp.int32), -1)
    token_start = jnp.take_along_axis(starts, segment, 1)
    token_cols = jnp.take_along_axis(columns, segment, 1)
    local = token_ids[None, :] - token_start
    row_place = local // (token_cols + 1)
    col_place = local % (token_cols + 1)
    return jnp.stack([row_place, col_place], 0).reshape(2, N_DP * SEQ).astype(jnp.int32)


def place_ends(drawn, own_key, smallest, largest):
    longest = drawn.shape.index(max(drawn.shape))
    spots = []
    for shift in (0, 1):
        where = [jax.random.randint(jax.random.fold_in(own_key, axis), (), 0, length) for axis, length in enumerate(drawn.shape)]
        where[longest] = (where[longest] + shift) % drawn.shape[longest]
        spots.append(tuple(where))
    return drawn.at[spots[0]].set(smallest).at[spots[1]].set(largest)


def spiked(entries, own_key, source, target, parts, factor):
    def block_of(dim):
        return (jnp.arange(entries.shape[dim]) // (entries.shape[dim] // parts)).reshape((-1,) + (1,) * (entries.ndim - 1 - dim))

    near = jax.random.permutation(own_key, parts)[block_of(target)]
    second = (block_of(target) + parts // 2) % parts
    return jnp.where((block_of(source) == near) | (block_of(source) == second), factor * entries, entries)


def level_of(stream_key, dims, cuts, smallest, top_value):
    def one(axis_at, shards_of):
        draws = jax.random.uniform(jax.random.fold_in(jax.random.fold_in(stream_key, 6), axis_at), (shards_of,), jnp.float32, smallest / len(cuts), top_value / len(cuts))
        return jnp.repeat(jnp.exp(draws), dims[axis_at] // shards_of).reshape((-1,) + (1,) * (len(dims) - axis_at - 1))

    level = one(*cuts[0])
    for cut in cuts[1:]:
        level = level * one(*cut)
    return level


def gaussian(own_key, shape, width, reach, cuts=(), held_as=jnp.bfloat16):
    loudness = level_of(own_key, shape, cuts, -0.22, 0.18) if cuts else 1.0
    drawn = jax.random.normal(own_key, shape, jnp.float32) * width * loudness
    return jnp.minimum(jnp.maximum(drawn, -reach), reach).astype(held_as)


def bell_draw_with(stream_key, extent, scale, reach, shards, heavy, kind=jnp.bfloat16):
    entries = scale * jax.random.normal(stream_key, extent, jnp.float32)
    if shards:
        entries = entries * level_of(stream_key, extent, shards, -0.22, 0.18)
    return jnp.clip(spiked(entries, jax.random.fold_in(stream_key, 3), *heavy), -reach, reach).astype(kind)


def setup_inputs(seed: int = 0) -> dict:
    streams_of = jax.random.split(jax.random.key(seed), 20)
    return {
        "hidden_in": gaussian(streams_of[0], (TOKENS, D), 1.0, 6.0, ((0, 32),)),
        "text_states": gaussian(streams_of[1], (TEXT_ROWS, TD), 1.0, 6.0, ((0, 8),)),
        "modulation": gaussian(streams_of[2], (N_DP, IMGS, 4 * D), 0.5, 3.0, ((0, 8),), jnp.float32),
        "image_lengths": draw_image_lengths(jax.random.fold_in(streams_of[19], 71), 0),
        "text_lengths": place_ends(jax.random.randint(streams_of[4], (N_DP, IMGS), TXT // 8, TXT + 1), jax.random.fold_in(streams_of[4], 1), TXT // 8, TXT).astype(jnp.int32),
        "positions": draw_positions(jax.random.fold_in(streams_of[19], 71), 0),
        "w_query": gaussian(streams_of[6], (D, D), D ** -0.5, 0.15625, ((1, 4),)),
        "w_key": gaussian(streams_of[7], (D, D), D ** -0.5, 0.15625, ((1, 4),)),
        "w_value": gaussian(streams_of[8], (D, D), D ** -0.5, 0.15625, ((1, 4),)),
        "w_out": gaussian(streams_of[9], (D, D), (D // 16) ** -0.5, 0.625, ((0, 4),)),
        "w_text_key": gaussian(streams_of[10], (TD, D), TD ** -0.5, 0.09375, ((1, 4),)),
        "w_text_value": gaussian(streams_of[11], (TD, D), TD ** -0.5, 0.09375, ((1, 4),)),
        "w_gate": gaussian(streams_of[12], (D, FF), D ** -0.5, 0.15625, ((1, 4),)),
        "w_up": gaussian(streams_of[13], (D, FF), D ** -0.5, 0.15625, ((1, 4),)),
        "w_down": gaussian(streams_of[14], (FF, D), FF ** -0.5, 0.09375, ((0, 4),)),
        "attention_gain": jnp.clip(1.0 + 0.1 * jax.random.normal(streams_of[15], (D,), jnp.float32), 0.5, 1.5),
        "feedforward_gain": jnp.clip(1.0 + 0.1 * jax.random.normal(streams_of[16], (D,), jnp.float32), 0.5, 1.5),
        "head_gates": jnp.clip(jax.random.uniform(streams_of[17], (H,), jnp.float32, 0.3, 1.2), 0.3, 1.2),
        "out_cotangent": bell_draw_with(streams_of[18], (TOKENS, D), 1.0, 6.0, ((0, 32),), (0, 1, 32, 2.75)),
    }


@jax.custom_vjp
def low(v):
    return lax.optimization_barrier(v.astype(jnp.bfloat16)).astype(jnp.float32)

@jax.custom_vjp
def low_back(v):
    return v

def low_keep(v):
    return (low(v), None)

def low_pass(kept, grad):
    return (grad,)

def back_keep(v):
    return (v, None)

def back_low(kept, grad):
    return (low(grad),)
low.defvjp(low_keep, low_pass)
low_back.defvjp(back_keep, back_low)

def product(left, right):
    return jnp.dot(left, right, precision=lax.Precision.HIGHEST)

def rope_tables(places, quarter):
    frequency = 10000.0 ** (-jnp.arange(quarter, dtype=jnp.float32) / quarter)
    angle_row = places[0].astype(jnp.float32)[:, None] * frequency[None, :]
    angle_col = places[1].astype(jnp.float32)[:, None] * frequency[None, :]
    return (jnp.cos(angle_row)[:, None, :], jnp.sin(angle_row)[:, None, :], jnp.cos(angle_col)[:, None, :], jnp.sin(angle_col)[:, None, :])

def rotate(values, tables):
    cos_row, sin_row, cos_col, sin_col = tables
    quarter = values.shape[-1] // 4
    part_one = values[..., 0:quarter]
    part_two = values[..., quarter:2 * quarter]
    part_three = values[..., 2 * quarter:3 * quarter]
    part_four = values[..., 3 * quarter:]
    return jnp.concatenate([part_one * cos_row - part_two * sin_row, part_two * cos_row + part_one * sin_row, part_three * cos_col - part_four * sin_col, part_four * cos_col + part_three * sin_col], -1)

def head_norm(values):
    return values * lax.rsqrt(lax.optimization_barrier(jnp.mean(values * values, -1, keepdims=True)) + 1e-06)

def modulated_norm(row_block, gain_vec, scale_vec):
    return row_block * lax.rsqrt(lax.optimization_barrier(jnp.mean(row_block * row_block, -1, keepdims=True)) + 1e-05) * gain_vec * (1.0 + scale_vec)

def attend(q_head, k_head, v_head, allowed):
    scores = low_back(product(q_head, k_head.T) * HD ** (-0.5))
    scores = jnp.where(allowed, scores, -1e+30)
    row_peak = lax.optimization_barrier(jnp.max(scores, -1, keepdims=True))
    exp_scores = jnp.exp(scores - row_peak)
    attention_probs = exp_scores / lax.optimization_barrier(jnp.sum(exp_scores, -1, keepdims=True))
    return low_back(product(low(attention_probs), v_head))

def forward_pack(hidden, mod_rows, weights, text_rows, image_of, allow_cross, tables):
    w_query, w_key, w_value, w_out, w_text_key, w_text_value, w_gate, w_up, w_down, attention_gain, feedforward_gain, head_gates = weights
    seq_len = hidden.shape[0]
    slot_count = text_rows.shape[0]
    select = (image_of[:, None] == jnp.arange(IMGS, dtype=jnp.int32)[None, :]).astype(jnp.float32)
    per_token = product(select, mod_rows)
    scale_attn = per_token[:, 0:D]
    gate_attn = per_token[:, D:2 * D]
    scale_ffn = per_token[:, 2 * D:3 * D]
    gate_ffn = per_token[:, 3 * D:]
    normed_one = low(modulated_norm(hidden, attention_gain, scale_attn))
    query_raw = low_back(product(normed_one, w_query))
    key_raw = low_back(product(normed_one, w_key))
    value_raw = low_back(product(normed_one, w_value))
    query_rot = low(rotate(head_norm(query_raw.reshape(seq_len, H, HD)), tables))
    key_rot = low(rotate(head_norm(key_raw.reshape(seq_len, H, HD)), tables))
    value_low = low(value_raw.reshape(seq_len, H, HD))
    text_key = low_back(product(text_rows, w_text_key))
    text_value = low_back(product(text_rows, w_text_value))
    text_key_low = low(head_norm(text_key.reshape(slot_count, H, HD)))
    text_value_low = low(text_value.reshape(slot_count, H, HD))
    allow_self = image_of[:, None] == image_of[None, :]

    def one_head(pieces):
        q_head, k_head, v_head, tk_head, tv_head, gate_head = pieces
        self_part = attend(q_head, k_head, v_head, allow_self)
        cross_part = attend(q_head, tk_head, tv_head, allow_cross)
        return low(self_part + jnp.tanh(gate_head) * cross_part)
    mixed_heads = lax.map(jax.checkpoint(one_head), (query_rot.transpose(1, 0, 2), key_rot.transpose(1, 0, 2), value_low.transpose(1, 0, 2), text_key_low.transpose(1, 0, 2), text_value_low.transpose(1, 0, 2), head_gates))
    mixed_heads = mixed_heads.transpose(1, 0, 2).reshape(seq_len, H * HD)
    attention_out = low_back(product(mixed_heads, w_out))
    after_attn = hidden + jnp.tanh(gate_attn) * attention_out
    normed_two = low(modulated_norm(after_attn, feedforward_gain, scale_ffn))
    gate_pre = low_back(product(normed_two, w_gate))
    up_pre = low_back(product(normed_two, w_up))
    inner_act = low(jax.nn.silu(gate_pre) * up_pre)
    ffn_out = low_back(product(inner_act, w_down))
    return after_attn + jnp.tanh(gate_ffn) * ffn_out

def reference(hidden_in, text_states, modulation, image_lengths, text_lengths, positions, w_query, w_key, w_value, w_out, w_text_key, w_text_value, w_gate, w_up, w_down, attention_gain, feedforward_gain, head_gates, out_cotangent):
    packs = image_lengths.shape[0]
    seq_len = hidden_in.shape[0] // packs
    slot_count = text_states.shape[0] // packs
    weights = tuple((matrix.astype(jnp.float32) for matrix in (w_query, w_key, w_value, w_out, w_text_key, w_text_value, w_gate, w_up, w_down, attention_gain, feedforward_gain, head_gates)))
    slot_ids = jnp.arange(slot_count, dtype=jnp.int32)
    slot_image = slot_ids // TXT
    slot_place = slot_ids % TXT
    image_ids = jnp.arange(IMGS, dtype=jnp.int32)
    token_ids = jnp.arange(seq_len, dtype=jnp.int32)

    def pack_step(running, pack_data):
        hidden, text_rows, mod_rows, lengths, text_limits, places, cotangent = pack_data
        image_ends = jnp.cumsum(lengths).astype(jnp.int32)
        image_of = lax.optimization_barrier(jnp.sum((token_ids[:, None] >= image_ends[None, :]).astype(jnp.int32), 1))
        slot_limit = lax.optimization_barrier(jnp.sum(jnp.where(slot_image[:, None] == image_ids[None, :], text_limits[None, :], 0), 1))
        allow_cross = (image_of[:, None] == slot_image[None, :]) & (slot_place < slot_limit)[None, :]
        tables = rope_tables(places, HD // 4)
        text_float = text_rows.astype(jnp.float32)

        def forward(hidden_float, mod_float, params):
            return forward_pack(hidden_float, mod_float, params, text_float, image_of, allow_cross, tables)
        output, back = jax.vjp(forward, hidden.astype(jnp.float32), mod_rows, weights)
        d_hidden, d_mod, d_weights = back(cotangent.astype(jnp.float32))
        running = jax.tree.map(lambda a, b: a + b, running, d_weights)
        return (running, (output.astype(jnp.bfloat16), d_hidden.astype(jnp.bfloat16), d_mod))
    zero_grads = jax.tree.map(jnp.zeros_like, weights)
    inputs = (hidden_in.reshape(packs, seq_len, D), text_states.reshape(packs, slot_count, TD), modulation, image_lengths, text_lengths, positions.reshape(2, packs, seq_len).transpose(1, 0, 2), out_cotangent.reshape(packs, seq_len, D))
    totals, (outputs, d_inputs, d_mods) = lax.scan(pack_step, zero_grads, inputs)
    return (outputs.reshape(packs * seq_len, D), d_inputs.reshape(packs * seq_len, D), d_mods, totals[0], totals[1], totals[2], totals[3], totals[4], totals[5], totals[6], totals[7], totals[8], totals[9], totals[10], totals[11])
```

```python
import functools

import jax
import jax.numpy as jnp
from jax import lax
from jax.experimental import pallas as pl
from jax.experimental.pallas import tpu as pltpu
from jax.sharding import PartitionSpec as P

D = 1536
H = 24
HD = 64
TXT = 256
IMGS = 5
LANES = 128
BQ = 256
BK = 256
SEG = HD
LSE = HD + IMGS
OFF = 256.0
NT = (((1,), (1,)), ((), ()))


def modulated_norm(row_block, gain_vec, scale_vec):
    return (
        row_block
        * lax.rsqrt(jnp.mean(row_block * row_block, -1, keepdims=True) + 1e-05)
        * gain_vec
        * (1.0 + scale_vec)
    )


def lane_of(rows):
    return lax.broadcasted_iota(jnp.int32, (rows, LANES), 1)


def first_head(lane):
    return lane < HD


def swap_quarters(x, lane):
    low = (lane % 32) < 16
    return jnp.where(low, pltpu.roll(x, LANES - 16, 1), pltpu.roll(x, 16, 1))


def half_sums(x, lane):
    one = jnp.sum(jnp.where(first_head(lane), x, 0.0), -1, keepdims=True)
    two = jnp.sum(jnp.where(first_head(lane), 0.0, x), -1, keepdims=True)
    return jnp.where(first_head(lane), one, two)


def normed_heads(x, lane):
    return x * lax.rsqrt(half_sums(x * x, lane) * (1.0 / HD) + 1e-06)


def normed_heads_back(x, w, lane):
    r = lax.rsqrt(half_sums(x * x, lane) * (1.0 / HD) + 1e-06)
    return r * (w - x * (r * r) * (half_sums(w * x, lane) * (1.0 / HD)))


def turned(y, cos, sin, lane):
    return y * cos + swap_quarters(y, lane) * sin


def turned_back(dy, cos, sin, lane):
    return dy * cos + swap_quarters(dy * sin, lane)


def three_parts(x):
    one = x.astype(jnp.bfloat16).astype(jnp.float32)
    two = (x - one).astype(jnp.bfloat16).astype(jnp.float32)
    return one, two, x - one - two


def with_parts(base, x, lane, at):
    one, two, three = three_parts(x)
    return jnp.where(
        lane == at, one, jnp.where(lane == at + 1, two, jnp.where(lane == at + 2, three, base))
    )


def attend_kernel(
    bounds,
    gates,
    q_ref,
    k_ref,
    v_ref,
    tk_ref,
    tv_ref,
    cosq_ref,
    sinq_ref,
    cos_ref,
    sin_ref,
    qm_ref,
    km_ref,
    tm_ref,
    mixed_ref,
    os_ref,
    oc_ref,
    qs_ref,
    qc_ref,
    kh_ref,
    vh_ref,
    tkh_ref,
    tvh_ref,
):
    pair, block = pl.program_id(0), pl.program_id(1)
    bf16, f32 = jnp.bfloat16, jnp.float32

    @pl.when(block == 0)
    def _():
        lane = lane_of(BK)
        ones = jnp.where((lane >= HD) & (lane < HD + 3), 1.0, 0.0)

        def split(into, rows, x, rest):
            into[0, rows, :] = jnp.where(first_head(lane), x, rest).astype(bf16)
            into[1, rows, :] = jnp.where(first_head(lane), pltpu.roll(x, HD, 1), rest).astype(bf16)

        @pl.loop(0, k_ref.shape[0] // BK)
        def _(i):
            rows = pl.ds(pl.multiple_of(i * BK, BK), BK)
            key = turned(normed_heads(k_ref[rows, :], lane), cos_ref[rows, :], sin_ref[rows, :], lane)
            split(kh_ref, rows, key, km_ref[rows, :].astype(f32))
            split(vh_ref, rows, v_ref[rows, :], ones)

        @pl.loop(0, tk_ref.shape[0] // BK)
        def _(i):
            rows = pl.ds(pl.multiple_of(i * BK, BK), BK)
            split(tkh_ref, rows, normed_heads(tk_ref[rows, :], lane), tm_ref[rows, :].astype(f32))
            split(tvh_ref, rows, tv_ref[rows, :], ones)

    lane = lane_of(BQ)
    query = turned(normed_heads(q_ref[...], lane), cosq_ref[...], sinq_ref[...], lane) * (HD**-0.5)
    extra = qm_ref[...].astype(f32)
    heads = (
        jnp.where(first_head(lane), query, extra).astype(bf16),
        jnp.where(first_head(lane), pltpu.roll(query, HD, 1), extra).astype(bf16),
    )

    def run(keys, values, start, stop):
        def body(j, accs):
            rows = pl.ds(pl.multiple_of(j * BK, BK), BK)
            new = []
            for i in range(2):
                scores = lax.dot_general(heads[i], keys[i, rows, :], NT, preferred_element_type=f32)
                probs = jnp.exp(scores).astype(bf16)
                new.append(accs[i] + jnp.dot(probs, values[i, rows, :], preferred_element_type=f32))
            return tuple(new)

        zero = jnp.zeros((BQ, LANES), f32)
        accs = lax.fori_loop(start, stop, body, (zero, zero))
        outs, totals = [], []
        for i in range(2):
            total = accs[i][:, HD : HD + 1]
            outs.append(accs[i] / total)
            totals.append(jnp.log(total))
        return outs, totals

    self_out, self_total = run(kh_ref, vh_ref, bounds[0, block], bounds[1, block])
    cross_out, cross_total = run(tkh_ref, tvh_ref, bounds[2, block], bounds[3, block])
    for i in range(2):
        wide = heads[i].astype(f32)
        qs_ref[i] = with_parts(wide, -self_total[i], lane, LSE).astype(bf16)
        qc_ref[i] = with_parts(wide, -cross_total[i], lane, LSE).astype(bf16)
    both_self = jnp.where(first_head(lane), self_out[0], pltpu.roll(self_out[1], HD, 1))
    both_cross = jnp.where(first_head(lane), cross_out[0], pltpu.roll(cross_out[1], HD, 1))
    gate = jnp.where(first_head(lane), gates[2 * pair], gates[2 * pair + 1])
    os_ref[...] = both_self
    oc_ref[...] = both_cross
    mixed_ref[...] = (both_self + gate * both_cross).astype(bf16)


def attend_back_kernel(
    bounds,
    gates,
    dm_ref,
    os_ref,
    oc_ref,
    qs_ref,
    qc_ref,
    kh_ref,
    vh_ref,
    tkh_ref,
    tvh_ref,
    q_ref,
    k_ref,
    tk_ref,
    cosq_ref,
    sinq_ref,
    cos_ref,
    sin_ref,
    dq_ref,
    dk_ref,
    dv_ref,
    dtk_ref,
    dtv_ref,
    dh_ref,
    dk_acc,
    dv_acc,
    dtk_acc,
    dtv_acc,
    kt,
    tkt,
):
    pair, block = pl.program_id(0), pl.program_id(1)
    bf16, f32 = jnp.bfloat16, jnp.float32

    @pl.when(block == 0)
    def _():
        for acc in (dk_acc, dv_acc, dtk_acc, dtv_acc):
            acc[...] = jnp.zeros_like(acc)
        dh_ref[...] = jnp.zeros_like(dh_ref)
        for i in range(2):
            kt[i] = kh_ref[i].T
            tkt[i] = tkh_ref[i].T

    lane = lane_of(BQ)
    gate = jnp.where(first_head(lane), gates[2 * pair], gates[2 * pair + 1])
    d_mixed = dm_ref[...]
    both_cross = oc_ref[...]
    dh_ref[...] += jnp.sum((d_mixed * both_cross).reshape(1, BQ // 8, 8, LANES), 1)

    def cotangents(d_out, out):
        d_out = d_out.astype(bf16).astype(f32)
        terms = d_out * out
        one = jnp.sum(jnp.where(first_head(lane), terms, 0.0), -1, keepdims=True)
        two = jnp.sum(jnp.where(first_head(lane), 0.0, terms), -1, keepdims=True)
        zero = jnp.zeros_like(d_out)
        return (
            with_parts(jnp.where(first_head(lane), d_out, zero), -one, lane, HD).astype(bf16),
            with_parts(
                jnp.where(first_head(lane), pltpu.roll(d_out, HD, 1), zero), -two, lane, HD
            ).astype(bf16),
        )

    d_self = cotangents(d_mixed, os_ref[...])
    d_cross = cotangents(gate * d_mixed, both_cross)

    def run(queries, d_outs, keys, values, keys_t, dk, dv, start, stop, accs):
        def body(j, accs):
            rows = pl.ds(pl.multiple_of(j * BK, BK), BK)
            new = []
            for i in range(2):
                query = queries[i]
                scores = lax.dot_general(keys[i, rows, :], query, NT, preferred_element_type=f32)
                d_probs = lax.dot_general(
                    values[i, rows, :], d_outs[i], NT, preferred_element_type=f32
                )
                probs = jnp.exp(scores)
                d_scores = (probs * d_probs).astype(bf16)
                dv[i, rows, :] += jnp.dot(
                    probs.astype(bf16), d_outs[i], preferred_element_type=f32
                )
                dk[i, rows, :] += jnp.dot(d_scores, query, preferred_element_type=f32)
                new.append(
                    accs[i]
                    + jnp.dot(keys_t[i, :, rows], d_scores, preferred_element_type=f32)
                )
            return tuple(new)

        return lax.fori_loop(start, stop, body, accs)

    zero = jnp.zeros((LANES, BQ), f32)
    accs = run(
        qs_ref, d_self, kh_ref, vh_ref, kt, dk_acc, dv_acc, bounds[0, block], bounds[1, block], (zero, zero)
    )
    accs = run(
        qc_ref, d_cross, tkh_ref, tvh_ref, tkt, dtk_acc, dtv_acc, bounds[2, block], bounds[3, block], accs
    )
    d_query = jnp.where(first_head(lane), accs[0].T, pltpu.roll(accs[1].T, HD, 1)) * (HD**-0.5)
    d_query = turned_back(d_query, cosq_ref[...], sinq_ref[...], lane)
    dq_ref[...] = normed_heads_back(q_ref[...], d_query, lane).astype(bf16)

    @pl.when(block == pl.num_programs(1) - 1)
    def _():
        lane = lane_of(BK)

        def joined(acc, rows):
            return jnp.where(first_head(lane), acc[0, rows, :], pltpu.roll(acc[1, rows, :], HD, 1))

        @pl.loop(0, k_ref.shape[0] // BK)
        def _(i):
            rows = pl.ds(pl.multiple_of(i * BK, BK), BK)
            d_key = turned_back(joined(dk_acc, rows), cos_ref[rows, :], sin_ref[rows, :], lane)
            dk_ref[rows, :] = normed_heads_back(k_ref[rows, :], d_key, lane).astype(bf16)
            dv_ref[rows, :] = joined(dv_acc, rows).astype(bf16)

        @pl.loop(0, tk_ref.shape[0] // BK)
        def _(i):
            rows = pl.ds(pl.multiple_of(i * BK, BK), BK)
            dtk_ref[rows, :] = normed_heads_back(
                tk_ref[rows, :], joined(dtk_acc, rows), lane
            ).astype(bf16)
            dtv_ref[rows, :] = joined(dtv_acc, rows).astype(bf16)


def window(rows, at):
    return pl.BlockSpec((rows, LANES), at)


def attend(bounds, gates, joint, text, cos, sin, qm, km, tm):
    seq, slots = joint.shape[0], text.shape[0]
    pairs = joint.shape[1] // (3 * LANES)
    blocks = seq // BQ
    bf16, f32 = jnp.bfloat16, jnp.float32
    per_head = lambda rows: pl.BlockSpec((2, rows, LANES), lambda p, b, *_: (p, 0, 0))
    grid = pltpu.PrefetchScalarGridSpec(
        num_scalar_prefetch=2,
        grid=(pairs, blocks),
        in_specs=[
            window(BQ, lambda p, b, *_: (b, p)),
            window(seq, lambda p, b, *_: (0, pairs + p)),
            window(seq, lambda p, b, *_: (0, 2 * pairs + p)),
            window(slots, lambda p, b, *_: (0, p)),
            window(slots, lambda p, b, *_: (0, pairs + p)),
            window(BQ, lambda p, b, *_: (b, 0)),
            window(BQ, lambda p, b, *_: (b, 0)),
            window(seq, lambda p, b, *_: (0, 0)),
            window(seq, lambda p, b, *_: (0, 0)),
            window(BQ, lambda p, b, *_: (b, 0)),
            window(seq, lambda p, b, *_: (0, 0)),
            window(slots, lambda p, b, *_: (0, 0)),
        ],
        out_specs=[
            window(BQ, lambda p, b, *_: (b, p)),
            window(BQ, lambda p, b, *_: (b, p)),
            window(BQ, lambda p, b, *_: (b, p)),
            pl.BlockSpec((2, BQ, LANES), lambda p, b, *_: (p, b, 0)),
            pl.BlockSpec((2, BQ, LANES), lambda p, b, *_: (p, b, 0)),
            per_head(seq),
            per_head(seq),
            per_head(slots),
            per_head(slots),
        ],
    )
    wide = pairs * LANES
    held = lambda rows: jax.ShapeDtypeStruct((2 * pairs, rows, LANES), bf16)
    return pl.pallas_call(
        attend_kernel,
        grid_spec=grid,
        out_shape=[
            jax.ShapeDtypeStruct((seq, wide), bf16),
            jax.ShapeDtypeStruct((seq, wide), f32),
            jax.ShapeDtypeStruct((seq, wide), f32),
            held(seq),
            held(seq),
            held(seq),
            held(seq),
            held(slots),
            held(slots),
        ],
        compiler_params=pltpu.CompilerParams(dimension_semantics=("arbitrary", "arbitrary")),
        cost_estimate=pl.CostEstimate(
            flops=20_000_000_000, bytes_accessed=30_000_000, transcendentals=0
        ),
        name="attend",
    )(bounds, gates, joint, joint, joint, text, text, cos, sin, cos, sin, qm, km, tm)


def attend_back(bounds, gates, d_mixed, saved, joint, text, cos, sin):
    seq, slots = joint.shape[0], text.shape[0]
    pairs = joint.shape[1] // (3 * LANES)
    blocks = seq // BQ
    bf16, f32 = jnp.bfloat16, jnp.float32
    per_head = lambda rows: pl.BlockSpec((2, rows, LANES), lambda p, b, *_: (p, 0, 0))
    per_block = pl.BlockSpec((2, BQ, LANES), lambda p, b, *_: (p, b, 0))
    mine = window(BQ, lambda p, b, *_: (b, p))
    grid = pltpu.PrefetchScalarGridSpec(
        num_scalar_prefetch=2,
        grid=(pairs, blocks),
        in_specs=[
            mine,
            mine,
            mine,
            per_block,
            per_block,
            per_head(seq),
            per_head(seq),
            per_head(slots),
            per_head(slots),
            mine,
            window(seq, lambda p, b, *_: (0, pairs + p)),
            window(slots, lambda p, b, *_: (0, p)),
            window(BQ, lambda p, b, *_: (b, 0)),
            window(BQ, lambda p, b, *_: (b, 0)),
            window(seq, lambda p, b, *_: (0, 0)),
            window(seq, lambda p, b, *_: (0, 0)),
        ],
        out_specs=[
            mine,
            window(seq, lambda p, b, *_: (0, p)),
            window(seq, lambda p, b, *_: (0, p)),
            window(slots, lambda p, b, *_: (0, p)),
            window(slots, lambda p, b, *_: (0, p)),
            pl.BlockSpec((1, 8, LANES), lambda p, b, *_: (p, 0, 0)),
        ],
        scratch_shapes=[
            pltpu.VMEM((2, seq, LANES), f32),
            pltpu.VMEM((2, seq, LANES), f32),
            pltpu.VMEM((2, slots, LANES), f32),
            pltpu.VMEM((2, slots, LANES), f32),
            pltpu.VMEM((2, LANES, seq), bf16),
            pltpu.VMEM((2, LANES, slots), bf16),
        ],
    )
    wide = pairs * LANES
    return pl.pallas_call(
        attend_back_kernel,
        grid_spec=grid,
        out_shape=[
            jax.ShapeDtypeStruct((seq, wide), bf16),
            jax.ShapeDtypeStruct((seq, wide), bf16),
            jax.ShapeDtypeStruct((seq, wide), bf16),
            jax.ShapeDtypeStruct((slots, wide), bf16),
            jax.ShapeDtypeStruct((slots, wide), bf16),
            jax.ShapeDtypeStruct((pairs, 8, LANES), f32),
        ],
        compiler_params=pltpu.CompilerParams(dimension_semantics=("arbitrary", "arbitrary")),
        cost_estimate=pl.CostEstimate(
            flops=60_000_000_000, bytes_accessed=40_000_000, transcendentals=0
        ),
        name="attend_back",
    )(
        bounds, gates, d_mixed, *saved, joint, joint, text, cos, sin, cos, sin
    )


def swapped(value, axis, bit):
    size = lax.axis_size(axis)
    return lax.ppermute(value, axis, [(i, i ^ bit) for i in range(size)])


def gather_rows(mine):
    size = lax.axis_size("mp")
    if size != 4:
        return lax.all_gather(mine, "mp", axis=0, tiled=True)
    rows, me = mine.shape[0], lax.axis_index("mp")
    across = swapped(mine, "mp", 2)
    beside = swapped(mine, "mp", 1)
    diagonal = swapped(across, "mp", 1)
    out = jnp.zeros((4, rows, mine.shape[1]), mine.dtype)
    for part, bit in ((mine, 0), (beside, 1), (across, 2), (diagonal, 3)):
        out = lax.dynamic_update_slice(out, part[None], (me ^ bit, 0, 0))
    return out.reshape(4 * rows, mine.shape[1])


def scatter_rows(partial):
    size = lax.axis_size("mp")
    if size != 4:
        return lax.psum_scatter(partial, "mp", scatter_dimension=0, tiled=True).astype(jnp.float32)
    me = lax.axis_index("mp")
    quarters = partial.reshape(4, partial.shape[0] // 4, partial.shape[1])
    take = lambda bit: lax.dynamic_index_in_dim(quarters, me ^ bit, 0, keepdims=False)
    far = swapped(take(3), "mp", 1)
    near = swapped(take(1), "mp", 1)
    summed = (take(2).astype(jnp.float32) + far.astype(jnp.float32)).astype(jnp.bfloat16)
    other = swapped(summed, "mp", 2)
    return take(0).astype(jnp.float32) + near.astype(jnp.float32) + other.astype(jnp.float32)


def sum_over(value, axes):
    for axis in axes:
        bit = 1
        while bit < lax.axis_size(axis):
            value = value + swapped(value, axis, bit)
            bit *= 2
    return value


def on_device(
    hidden_in,
    text_states,
    modulation,
    image_lengths,
    text_lengths,
    positions,
    w_query,
    w_key,
    w_value,
    w_out,
    w_text_key,
    w_text_value,
    w_gate,
    w_up,
    w_down,
    attention_gain,
    feedforward_gain,
    head_gates,
    out_cotangent,
):
    highest = lax.Precision.HIGHEST
    bf16, f32 = jnp.bfloat16, jnp.float32
    contract_rows = (((0,), (0,)), ((), ()))
    contract_cols = (((1,), (1,)), ((), ()))
    local_rows = hidden_in.shape[0]
    shard_index = lax.axis_index("mp")
    seq_len = local_rows * lax.axis_size("mp")
    local_heads = w_query.shape[1] // HD
    local_width = local_heads * HD
    wide = -(-local_width // LANES) * LANES
    spare = wide - local_width
    slot_count = text_states.shape[0]
    image_ids = jnp.arange(IMGS, dtype=jnp.int32)
    token_ids = jnp.arange(seq_len, dtype=jnp.int32)
    image_ends = jnp.cumsum(image_lengths[0])
    image_starts = image_ends - image_lengths[0]
    image_of = jnp.sum((token_ids[:, None] >= image_ends[None, :]).astype(jnp.int32), 1)
    select_all = (image_of[:, None] == image_ids[None, :]).astype(f32)
    select_mine = lax.dynamic_slice_in_dim(select_all, shard_index * local_rows, local_rows, 0)
    per_token = jnp.dot(select_mine, modulation[0], precision=highest)
    scale_attn = per_token[:, 0:D]
    gate_attn = per_token[:, D : 2 * D]
    scale_ffn = per_token[:, 2 * D : 3 * D]
    gate_ffn = per_token[:, 3 * D :]

    def lanes(columns):
        rows = columns.shape[0]
        return jnp.pad(columns, ((0, 0), (HD, LANES - HD - columns.shape[1]))).astype(bf16)

    slot_ids = jnp.arange(slot_count, dtype=jnp.int32)
    slot_live = (slot_ids % TXT)[:, None] < text_lengths[0][None, :]
    slot_fits = ((slot_ids // TXT)[:, None] == image_ids[None, :]) & slot_live
    three = lambda rows: jnp.ones((rows, 3), f32)
    query_lanes = lanes(select_all)
    key_lanes = lanes(jnp.concatenate([(select_all - 1.0) * OFF, three(seq_len)], 1))
    text_lanes = lanes(
        jnp.concatenate([jnp.where(slot_fits, 0.0, -OFF), three(slot_count)], 1)
    )
    block_first = jnp.arange(seq_len // BQ, dtype=jnp.int32) * BQ
    in_first = jnp.sum((block_first[:, None] >= image_ends[None, :]).astype(jnp.int32), 1)
    in_last = jnp.sum(((block_first + BQ - 1)[:, None] >= image_ends[None, :]).astype(jnp.int32), 1)
    pick = lambda values, at: jnp.sum(
        jnp.where(at[:, None] == image_ids[None, :], values[None, :], 0), 1
    )
    bounds = jnp.stack(
        [
            pick(image_starts, in_first) // BK,
            (pick(image_ends, in_last) + BK - 1) // BK,
            in_first,
            in_last + 1,
        ]
    ).astype(jnp.int32)

    quarter = HD // 4
    frequency = 10000.0 ** (-jnp.arange(quarter, dtype=f32) / quarter)
    angle_row = positions[0].astype(f32)[:, None] * frequency[None, :]
    angle_col = positions[1].astype(f32)[:, None] * frequency[None, :]
    cos_row, sin_row, cos_col, sin_col = (
        jnp.cos(angle_row),
        jnp.sin(angle_row),
        jnp.cos(angle_col),
        jnp.sin(angle_col),
    )
    cos = jnp.concatenate([cos_row, cos_row, cos_col, cos_col] * 2, 1)
    sin = jnp.concatenate([-sin_row, sin_row, -sin_col, sin_col] * 2, 1)

    hidden_float = hidden_in.astype(f32)
    normed_one, back_norm_one = jax.vjp(modulated_norm, hidden_float, attention_gain, scale_attn)
    rows_attn = gather_rows(normed_one.astype(bf16))
    tanh_ffn = jnp.tanh(gate_ffn)
    cotangent = out_cotangent.astype(f32)
    d_ffn_all = gather_rows((cotangent * tanh_ffn).astype(bf16))

    widen = lambda w: jnp.pad(w, ((0, 0), (0, spare))) if spare else w
    w_joint = jnp.concatenate([widen(w_query), widen(w_key), widen(w_value)], 1)
    w_text = jnp.concatenate([widen(w_text_key), widen(w_text_value)], 1)
    w_out_wide = jnp.pad(w_out, ((0, spare), (0, 0))) if spare else w_out
    text_joint = jnp.dot(text_states, w_text, preferred_element_type=f32)
    joint = jnp.dot(rows_attn, w_joint, preferred_element_type=f32)
    gate_mine = lax.dynamic_slice_in_dim(head_gates, shard_index * local_heads, local_heads, 0)
    gate_tanh = jnp.tanh(gate_mine)
    gates = jnp.pad(gate_tanh, (0, wide // HD - local_heads))
    mixed_low, *saved = attend(
        bounds, gates, joint, text_joint, cos, sin, query_lanes, key_lanes, text_lanes
    )

    attention_out = scatter_rows(jnp.dot(mixed_low, w_out_wide, preferred_element_type=f32).astype(bf16))
    tanh_attn = jnp.tanh(gate_attn)
    after_attn = hidden_float + tanh_attn * attention_out
    normed_two, back_norm_two = jax.vjp(modulated_norm, after_attn, feedforward_gain, scale_ffn)
    rows_ffn = gather_rows(normed_two.astype(bf16))
    gate_pre = jnp.dot(rows_ffn, w_gate, preferred_element_type=f32)
    up_pre = jnp.dot(rows_ffn, w_up, preferred_element_type=f32)
    sigmoid_gate = jax.nn.sigmoid(gate_pre)
    activated = gate_pre * sigmoid_gate
    inner_low = (activated * up_pre).astype(bf16)
    d_inner = lax.dot_general(d_ffn_all, w_down, contract_cols, preferred_element_type=f32)
    d_gate_low = (d_inner * up_pre * sigmoid_gate * (1.0 + gate_pre * (1.0 - sigmoid_gate))).astype(
        bf16
    )
    d_up_low = (d_inner * activated).astype(bf16)
    d_normed_two = scatter_rows(
        (
            lax.dot_general(d_gate_low, w_gate, contract_cols, preferred_element_type=f32)
            + lax.dot_general(d_up_low, w_up, contract_cols, preferred_element_type=f32)
        ).astype(bf16)
    )
    ffn_out = scatter_rows(jnp.dot(inner_low, w_down, preferred_element_type=f32).astype(bf16))
    block_out = (after_attn + tanh_ffn * ffn_out).astype(bf16)
    d_gate_ffn = cotangent * ffn_out * (1.0 - tanh_ffn * tanh_ffn)
    grad_down_t = lax.dot_general(d_ffn_all, inner_low, contract_rows, preferred_element_type=f32)
    grad_gate = lax.dot_general(rows_ffn, d_gate_low, contract_rows, preferred_element_type=f32)
    grad_up = lax.dot_general(rows_ffn, d_up_low, contract_rows, preferred_element_type=f32)

    def sum_packs(*grads):
        joined = jnp.concatenate([g.astype(bf16) for g in grads], 1)
        summed = lax.psum_scatter(joined, "dp", scatter_dimension=0, tiled=True).astype(f32)
        parts, at = [], 0
        for g in grads:
            parts.append(summed[:, at : at + g.shape[1]])
            at += g.shape[1]
        return parts

    out_gate, out_up, out_down_t = sum_packs(grad_gate, grad_up, grad_down_t)

    d_after_norm, grad_ffn_gain, d_scale_ffn = back_norm_two(d_normed_two)
    d_after = cotangent + d_after_norm
    d_attn_low = (d_after * tanh_attn).astype(bf16)
    d_gate_attn = d_after * attention_out * (1.0 - tanh_attn * tanh_attn)
    d_attn_all = gather_rows(d_attn_low)
    grad_out_t = lax.dot_general(d_attn_all, mixed_low, contract_rows, preferred_element_type=f32)
    d_mixed = lax.dot_general(d_attn_all, w_out_wide, contract_cols, preferred_element_type=f32)
    d_query, d_key, d_value, d_text_key, d_text_value, d_heads = attend_back(
        bounds, gates, d_mixed, saved, joint, text_joint, cos, sin
    )
    grad_heads = jnp.sum(d_heads, 1).reshape(wide // HD, HD).sum(1)[:local_heads]
    grad_heads = grad_heads * (1.0 - gate_tanh * gate_tanh)
    narrow = lambda d: d[:, :local_width]
    d_text_low = jnp.concatenate([narrow(d_text_key), narrow(d_text_value)], 1)
    grad_text = lax.dot_general(text_states, d_text_low, contract_rows, preferred_element_type=f32)
    (out_text,) = sum_packs(grad_text)
    d_joint_low = jnp.concatenate([d_query, d_key, d_value], 1)
    d_normed_one = scatter_rows(
        lax.dot_general(d_joint_low, w_joint, contract_cols, preferred_element_type=f32).astype(bf16)
    )
    d_joint_low = jnp.concatenate([narrow(d_query), narrow(d_key), narrow(d_value)], 1)
    grad_joint = lax.dot_general(rows_attn, d_joint_low, contract_rows, preferred_element_type=f32)
    out_joint, out_out_t = sum_packs(grad_joint, narrow(grad_out_t))

    d_hidden_norm, grad_attn_gain, d_scale_attn = back_norm_one(d_normed_one)
    input_grad = (d_after + d_hidden_norm).astype(bf16)
    d_per_token = jnp.concatenate([d_scale_attn, d_gate_attn, d_scale_ffn, d_gate_ffn], 1)
    mod_partial = lax.dot_general(select_mine, d_per_token, contract_rows, precision=highest)
    modulation_grad = sum_over(mod_partial, ("mp",))[None]
    heads_full = lax.dynamic_update_slice(
        jnp.zeros((H,), f32), grad_heads, (shard_index * local_heads,)
    )
    small = jnp.concatenate([grad_attn_gain, grad_ffn_gain, heads_full])
    small = sum_over(small, ("mp", "dp"))
    return (
        block_out,
        input_grad,
        modulation_grad,
        out_joint[:, 0:local_width],
        out_joint[:, local_width : 2 * local_width],
        out_joint[:, 2 * local_width :],
        out_out_t.T,
        out_text[:, 0:local_width],
        out_text[:, local_width:],
        out_gate,
        out_up,
        out_down_t.T,
        small[0:D],
        small[D : 2 * D],
        small[2 * D :],
    )


def solution(mesh):
    placed = (
        P(("dp", "mp"), None),
        P("dp", None),
        P("dp", None, None),
        P("dp", None),
        P("dp", None),
        P(None, "dp"),
        P(None, "mp"),
        P(None, "mp"),
        P(None, "mp"),
        P("mp", None),
        P(None, "mp"),
        P(None, "mp"),
        P(None, "mp"),
        P(None, "mp"),
        P("mp", None),
        P(),
        P(),
        P(),
        P(("dp", "mp"), None),
    )
    return jax.shard_map(
        on_device,
        mesh=mesh,
        in_specs=placed,
        out_specs=(
            P(("dp", "mp"), None),
            P(("dp", "mp"), None),
            P("dp", None, None),
            P("dp", "mp"),
            P("dp", "mp"),
            P("dp", "mp"),
            P("mp", "dp"),
            P("dp", "mp"),
            P("dp", "mp"),
            P("dp", "mp"),
            P("dp", "mp"),
            P("mp", "dp"),
            P(),
            P(),
            P(),
        ),
        check_vma=False,
    )
```

```python
import functools

import jax
import jax.numpy as jnp
from jax import lax
from jax.experimental import pallas as pl
from jax.experimental.pallas import tpu as pltpu
from jax.sharding import PartitionSpec as P

D = 1536
H = 24
HD = 64
TXT = 256
IMGS = 5
LANES = 128
BQ = 256
BK = 256
SEG = HD
LSE = HD + IMGS
OFF = 256.0
NT = (((1,), (1,)), ((), ()))


def modulated_norm(row_block, gain_vec, scale_vec):
    return (
        row_block
        * lax.rsqrt(jnp.mean(row_block * row_block, -1, keepdims=True) + 1e-05)
        * gain_vec
        * (1.0 + scale_vec)
    )


def lane_of(rows):
    return lax.broadcasted_iota(jnp.int32, (rows, LANES), 1)


def first_head(lane):
    return lane < HD


def swap_quarters(x, lane):
    low = (lane % 32) < 16
    return jnp.where(low, pltpu.roll(x, LANES - 16, 1), pltpu.roll(x, 16, 1))


def half_sums(x, lane):
    one = jnp.sum(jnp.where(first_head(lane), x, 0.0), -1, keepdims=True)
    two = jnp.sum(jnp.where(first_head(lane), 0.0, x), -1, keepdims=True)
    return jnp.where(first_head(lane), one, two)


def normed_heads(x, lane):
    return x * lax.rsqrt(half_sums(x * x, lane) * (1.0 / HD) + 1e-06)


def normed_heads_back(x, w, lane):
    r = lax.rsqrt(half_sums(x * x, lane) * (1.0 / HD) + 1e-06)
    return r * (w - x * (r * r) * (half_sums(w * x, lane) * (1.0 / HD)))


def turned(y, cos, sin, lane):
    return y * cos + swap_quarters(y, lane) * sin


def turned_back(dy, cos, sin, lane):
    return dy * cos + swap_quarters(dy * sin, lane)


def three_parts(x):
    one = x.astype(jnp.bfloat16).astype(jnp.float32)
    two = (x - one).astype(jnp.bfloat16).astype(jnp.float32)
    return one, two, x - one - two


def with_parts(base, x, lane, at):
    one, two, three = three_parts(x)
    return jnp.where(
        lane == at, one, jnp.where(lane == at + 1, two, jnp.where(lane == at + 2, three, base))
    )


def attend_kernel(
    bounds,
    gates,
    q_ref,
    k_ref,
    v_ref,
    tk_ref,
    tv_ref,
    cosq_ref,
    sinq_ref,
    cos_ref,
    sin_ref,
    qm_ref,
    km_ref,
    tm_ref,
    mixed_ref,
    os_ref,
    oc_ref,
    qs_ref,
    qc_ref,
    kh_ref,
    vh_ref,
    tkh_ref,
    tvh_ref,
):
    pair, block = pl.program_id(0), pl.program_id(1)
    bf16, f32 = jnp.bfloat16, jnp.float32

    @pl.when(block == 0)
    def _():
        lane = lane_of(BK)
        ones = jnp.where((lane >= HD) & (lane < HD + 3), 1.0, 0.0)

        def split(into, rows, x, rest):
            into[0, rows, :] = jnp.where(first_head(lane), x, rest).astype(bf16)
            into[1, rows, :] = jnp.where(first_head(lane), pltpu.roll(x, HD, 1), rest).astype(bf16)

        @pl.loop(0, k_ref.shape[0] // BK)
        def _(i):
            rows = pl.ds(pl.multiple_of(i * BK, BK), BK)
            held = pl.ds(pl.multiple_of(bounds[4, i] * BK, BK), BK)
            key = turned(normed_heads(k_ref[held, :], lane), cos_ref[rows, :], sin_ref[rows, :], lane)
            split(kh_ref, rows, key, km_ref[rows, :].astype(f32))
            split(vh_ref, rows, v_ref[held, :], ones)

        @pl.loop(0, tk_ref.shape[0] // BK)
        def _(i):
            rows = pl.ds(pl.multiple_of(i * BK, BK), BK)
            split(tkh_ref, rows, normed_heads(tk_ref[rows, :], lane), tm_ref[rows, :].astype(f32))
            split(tvh_ref, rows, tv_ref[rows, :], ones)

    lane = lane_of(BQ)
    query = turned(normed_heads(q_ref[...], lane), cosq_ref[...], sinq_ref[...], lane) * (HD**-0.5)
    extra = qm_ref[...].astype(f32)
    heads = (
        jnp.where(first_head(lane), query, extra).astype(bf16),
        jnp.where(first_head(lane), pltpu.roll(query, HD, 1), extra).astype(bf16),
    )

    def run(keys, values, start, stop):
        def body(j, accs):
            rows = pl.ds(pl.multiple_of(j * BK, BK), BK)
            new = []
            for i in range(2):
                scores = lax.dot_general(heads[i], keys[i, rows, :], NT, preferred_element_type=f32)
                probs = jnp.exp(scores).astype(bf16)
                new.append(accs[i] + jnp.dot(probs, values[i, rows, :], preferred_element_type=f32))
            return tuple(new)

        zero = jnp.zeros((BQ, LANES), f32)
        accs = lax.fori_loop(start, stop, body, (zero, zero))
        outs, totals = [], []
        for i in range(2):
            total = accs[i][:, HD : HD + 1]
            outs.append(accs[i] / total)
            totals.append(jnp.log(total))
        return outs, totals

    self_out, self_total = run(kh_ref, vh_ref, bounds[0, block], bounds[1, block])
    cross_out, cross_total = run(tkh_ref, tvh_ref, bounds[2, block], bounds[3, block])
    for i in range(2):
        wide = heads[i].astype(f32)
        qs_ref[i] = with_parts(wide, -self_total[i], lane, LSE).astype(bf16)
        qc_ref[i] = with_parts(wide, -cross_total[i], lane, LSE).astype(bf16)
    both_self = jnp.where(first_head(lane), self_out[0], pltpu.roll(self_out[1], HD, 1))
    both_cross = jnp.where(first_head(lane), cross_out[0], pltpu.roll(cross_out[1], HD, 1))
    gate = jnp.where(first_head(lane), gates[2 * pair], gates[2 * pair + 1])
    os_ref[...] = both_self
    oc_ref[...] = both_cross
    mixed_ref[...] = (both_self + gate * both_cross).astype(bf16)


def attend_back_kernel(
    bounds,
    gates,
    dm_ref,
    os_ref,
    oc_ref,
    qs_ref,
    qc_ref,
    kh_ref,
    vh_ref,
    tkh_ref,
    tvh_ref,
    q_ref,
    k_ref,
    tk_ref,
    cosq_ref,
    sinq_ref,
    cos_ref,
    sin_ref,
    dq_ref,
    dk_ref,
    dv_ref,
    dtk_ref,
    dtv_ref,
    dh_ref,
    dk_acc,
    dv_acc,
    dtk_acc,
    dtv_acc,
    kt,
    tkt,
):
    pair, block = pl.program_id(0), pl.program_id(1)
    bf16, f32 = jnp.bfloat16, jnp.float32

    @pl.when(block == 0)
    def _():
        for acc in (dk_acc, dv_acc, dtk_acc, dtv_acc):
            acc[...] = jnp.zeros_like(acc)
        dh_ref[...] = jnp.zeros_like(dh_ref)
        for i in range(2):
            kt[i] = kh_ref[i].T
            tkt[i] = tkh_ref[i].T

    lane = lane_of(BQ)
    gate = jnp.where(first_head(lane), gates[2 * pair], gates[2 * pair + 1])
    d_mixed = dm_ref[...]
    both_cross = oc_ref[...]
    dh_ref[...] += jnp.sum((d_mixed * both_cross).reshape(1, BQ // 8, 8, LANES), 1)

    def cotangents(d_out, out):
        d_out = d_out.astype(bf16).astype(f32)
        terms = d_out * out
        one = jnp.sum(jnp.where(first_head(lane), terms, 0.0), -1, keepdims=True)
        two = jnp.sum(jnp.where(first_head(lane), 0.0, terms), -1, keepdims=True)
        zero = jnp.zeros_like(d_out)
        return (
            with_parts(jnp.where(first_head(lane), d_out, zero), -one, lane, HD).astype(bf16),
            with_parts(
                jnp.where(first_head(lane), pltpu.roll(d_out, HD, 1), zero), -two, lane, HD
            ).astype(bf16),
        )

    d_self = cotangents(d_mixed, os_ref[...])
    d_cross = cotangents(gate * d_mixed, both_cross)

    def run(queries, d_outs, keys, values, keys_t, dk, dv, start, stop, accs):
        def body(j, accs):
            rows = pl.ds(pl.multiple_of(j * BK, BK), BK)
            new = []
            for i in range(2):
                query = queries[i]
                scores = lax.dot_general(keys[i, rows, :], query, NT, preferred_element_type=f32)
                d_probs = lax.dot_general(
                    values[i, rows, :], d_outs[i], NT, preferred_element_type=f32
                )
                probs = jnp.exp(scores)
                d_scores = (probs * d_probs).astype(bf16)
                dv[i, rows, :] += jnp.dot(
                    probs.astype(bf16), d_outs[i], preferred_element_type=f32
                )
                dk[i, rows, :] += jnp.dot(d_scores, query, preferred_element_type=f32)
                new.append(
                    accs[i]
                    + jnp.dot(keys_t[i, :, rows], d_scores, preferred_element_type=f32)
                )
            return tuple(new)

        return lax.fori_loop(start, stop, body, accs)

    zero = jnp.zeros((LANES, BQ), f32)
    accs = run(
        qs_ref, d_self, kh_ref, vh_ref, kt, dk_acc, dv_acc, bounds[0, block], bounds[1, block], (zero, zero)
    )
    accs = run(
        qc_ref, d_cross, tkh_ref, tvh_ref, tkt, dtk_acc, dtv_acc, bounds[2, block], bounds[3, block], accs
    )
    d_query = jnp.where(first_head(lane), accs[0].T, pltpu.roll(accs[1].T, HD, 1)) * (HD**-0.5)
    d_query = turned_back(d_query, cosq_ref[...], sinq_ref[...], lane)
    dq_ref[...] = normed_heads_back(q_ref[...], d_query, lane).astype(bf16)

    @pl.when(block == pl.num_programs(1) - 1)
    def _():
        lane = lane_of(BK)

        def joined(acc, rows):
            return jnp.where(first_head(lane), acc[0, rows, :], pltpu.roll(acc[1, rows, :], HD, 1))

        @pl.loop(0, k_ref.shape[0] // BK)
        def _(i):
            rows = pl.ds(pl.multiple_of(i * BK, BK), BK)
            held = pl.ds(pl.multiple_of(bounds[4, i] * BK, BK), BK)
            d_key = turned_back(joined(dk_acc, rows), cos_ref[rows, :], sin_ref[rows, :], lane)
            dk_ref[held, :] = normed_heads_back(k_ref[held, :], d_key, lane).astype(bf16)
            dv_ref[held, :] = joined(dv_acc, rows).astype(bf16)

        @pl.loop(0, tk_ref.shape[0] // BK)
        def _(i):
            rows = pl.ds(pl.multiple_of(i * BK, BK), BK)
            dtk_ref[rows, :] = normed_heads_back(
                tk_ref[rows, :], joined(dtk_acc, rows), lane
            ).astype(bf16)
            dtv_ref[rows, :] = joined(dtv_acc, rows).astype(bf16)


def window(rows, at):
    return pl.BlockSpec((rows, LANES), at)


def attend(bounds, gates, joint, text, cos, sin, qm, km, tm):
    seq, slots = joint.shape[0], text.shape[0]
    pairs = joint.shape[1] // (3 * LANES)
    blocks = seq // BQ
    bf16, f32 = jnp.bfloat16, jnp.float32
    per_head = lambda rows: pl.BlockSpec((2, rows, LANES), lambda p, b, *_: (p, 0, 0))
    grid = pltpu.PrefetchScalarGridSpec(
        num_scalar_prefetch=2,
        grid=(pairs, blocks),
        in_specs=[
            window(BQ, lambda p, b, at, *_: (at[4, b], p)),
            window(seq, lambda p, b, *_: (0, pairs + p)),
            window(seq, lambda p, b, *_: (0, 2 * pairs + p)),
            window(slots, lambda p, b, *_: (0, p)),
            window(slots, lambda p, b, *_: (0, pairs + p)),
            window(BQ, lambda p, b, *_: (b, 0)),
            window(BQ, lambda p, b, *_: (b, 0)),
            window(seq, lambda p, b, *_: (0, 0)),
            window(seq, lambda p, b, *_: (0, 0)),
            window(BQ, lambda p, b, *_: (b, 0)),
            window(seq, lambda p, b, *_: (0, 0)),
            window(slots, lambda p, b, *_: (0, 0)),
        ],
        out_specs=[
            window(BQ, lambda p, b, at, *_: (at[4, b], p)),
            window(BQ, lambda p, b, at, *_: (at[4, b], p)),
            window(BQ, lambda p, b, at, *_: (at[4, b], p)),
            pl.BlockSpec((2, BQ, LANES), lambda p, b, *_: (p, b, 0)),
            pl.BlockSpec((2, BQ, LANES), lambda p, b, *_: (p, b, 0)),
            per_head(seq),
            per_head(seq),
            per_head(slots),
            per_head(slots),
        ],
    )
    wide = pairs * LANES
    held = lambda rows: jax.ShapeDtypeStruct((2 * pairs, rows, LANES), bf16)
    return pl.pallas_call(
        attend_kernel,
        grid_spec=grid,
        out_shape=[
            jax.ShapeDtypeStruct((seq, wide), bf16),
            jax.ShapeDtypeStruct((seq, wide), f32),
            jax.ShapeDtypeStruct((seq, wide), f32),
            held(seq),
            held(seq),
            held(seq),
            held(seq),
            held(slots),
            held(slots),
        ],
        compiler_params=pltpu.CompilerParams(dimension_semantics=("arbitrary", "arbitrary")),
        cost_estimate=pl.CostEstimate(
            flops=20_000_000_000, bytes_accessed=30_000_000, transcendentals=0
        ),
        name="attend",
    )(bounds, gates, joint, joint, joint, text, text, cos, sin, cos, sin, qm, km, tm)


def attend_back(bounds, gates, d_mixed, saved, joint, text, cos, sin):
    seq, slots = joint.shape[0], text.shape[0]
    pairs = joint.shape[1] // (3 * LANES)
    blocks = seq // BQ
    bf16, f32 = jnp.bfloat16, jnp.float32
    per_head = lambda rows: pl.BlockSpec((2, rows, LANES), lambda p, b, *_: (p, 0, 0))
    per_block = pl.BlockSpec((2, BQ, LANES), lambda p, b, *_: (p, b, 0))
    mine = window(BQ, lambda p, b, at, *_: (at[4, b], p))
    grid = pltpu.PrefetchScalarGridSpec(
        num_scalar_prefetch=2,
        grid=(pairs, blocks),
        in_specs=[
            mine,
            mine,
            mine,
            per_block,
            per_block,
            per_head(seq),
            per_head(seq),
            per_head(slots),
            per_head(slots),
            mine,
            window(seq, lambda p, b, *_: (0, pairs + p)),
            window(slots, lambda p, b, *_: (0, p)),
            window(BQ, lambda p, b, *_: (b, 0)),
            window(BQ, lambda p, b, *_: (b, 0)),
            window(seq, lambda p, b, *_: (0, 0)),
            window(seq, lambda p, b, *_: (0, 0)),
        ],
        out_specs=[
            mine,
            window(seq, lambda p, b, *_: (0, p)),
            window(seq, lambda p, b, *_: (0, p)),
            window(slots, lambda p, b, *_: (0, p)),
            window(slots, lambda p, b, *_: (0, p)),
            pl.BlockSpec((1, 8, LANES), lambda p, b, *_: (p, 0, 0)),
        ],
        scratch_shapes=[
            pltpu.VMEM((2, seq, LANES), f32),
            pltpu.VMEM((2, seq, LANES), f32),
            pltpu.VMEM((2, slots, LANES), f32),
            pltpu.VMEM((2, slots, LANES), f32),
            pltpu.VMEM((2, LANES, seq), bf16),
            pltpu.VMEM((2, LANES, slots), bf16),
        ],
    )
    wide = pairs * LANES
    return pl.pallas_call(
        attend_back_kernel,
        grid_spec=grid,
        out_shape=[
            jax.ShapeDtypeStruct((seq, wide), bf16),
            jax.ShapeDtypeStruct((seq, wide), bf16),
            jax.ShapeDtypeStruct((seq, wide), bf16),
            jax.ShapeDtypeStruct((slots, wide), bf16),
            jax.ShapeDtypeStruct((slots, wide), bf16),
            jax.ShapeDtypeStruct((pairs, 8, LANES), f32),
        ],
        compiler_params=pltpu.CompilerParams(dimension_semantics=("arbitrary", "arbitrary")),
        cost_estimate=pl.CostEstimate(
            flops=60_000_000_000, bytes_accessed=40_000_000, transcendentals=0
        ),
        name="attend_back",
    )(
        bounds, gates, d_mixed, *saved, joint, joint, text, cos, sin, cos, sin
    )


def swapped(value, axis, bit):
    size = lax.axis_size(axis)
    return lax.ppermute(value, axis, [(i, i ^ bit) for i in range(size)])


def after(value, *others):
    return lax.optimization_barrier((value, *others))[0]


def near_rows(mine):
    return jnp.concatenate([mine, swapped(mine, "mp", 1)], 0)


def far_rows(mine, across):
    if across is None:
        return None
    return jnp.concatenate([across, swapped(across, "mp", 1)], 0)


def piece(half, at):
    rows = half.shape[0] // 2
    return half[at * rows : (at + 1) * rows]


def to_across(far):
    beside = swapped(piece(far, 1), "mp", 1)
    return (piece(far, 0).astype(jnp.float32) + beside.astype(jnp.float32)).astype(far.dtype)


def own_sum(near, other):
    beside = swapped(piece(near, 1), "mp", 1)
    total = piece(near, 0).astype(jnp.float32) + beside.astype(jnp.float32)
    return total + other.astype(jnp.float32)


def sum_over(value, axes):
    for axis in axes:
        bit = 1
        while bit < lax.axis_size(axis):
            value = value + swapped(value, axis, bit)
            bit *= 2
    return value


def on_device(
    hidden_in,
    text_states,
    modulation,
    image_lengths,
    text_lengths,
    positions,
    w_query,
    w_key,
    w_value,
    w_out,
    w_text_key,
    w_text_value,
    w_gate,
    w_up,
    w_down,
    attention_gain,
    feedforward_gain,
    head_gates,
    out_cotangent,
):
    highest = lax.Precision.HIGHEST
    bf16, f32 = jnp.bfloat16, jnp.float32
    contract_rows = (((0,), (0,)), ((), ()))
    contract_cols = (((1,), (1,)), ((), ()))
    local_rows = hidden_in.shape[0]
    shard_index = lax.axis_index("mp")
    seq_len = local_rows * lax.axis_size("mp")
    local_heads = w_query.shape[1] // HD
    local_width = local_heads * HD
    wide = -(-local_width // LANES) * LANES
    spare = wide - local_width
    slot_count = text_states.shape[0]
    hidden = w_gate.shape[1]
    halves = lax.axis_size("mp") == 4
    turn = shard_index if halves else jnp.int32(0)
    image_ids = jnp.arange(IMGS, dtype=jnp.int32)
    token_ids = jnp.arange(seq_len, dtype=jnp.int32)
    image_ends = jnp.cumsum(image_lengths[0])
    image_starts = image_ends - image_lengths[0]
    image_of = jnp.sum((token_ids[:, None] >= image_ends[None, :]).astype(jnp.int32), 1)
    select_all = (image_of[:, None] == image_ids[None, :]).astype(f32)
    select_mine = lax.dynamic_slice_in_dim(select_all, shard_index * local_rows, local_rows, 0)
    per_token = jnp.dot(select_mine, modulation[0], precision=highest)
    scale_attn = per_token[:, 0:D]
    gate_attn = per_token[:, D : 2 * D]
    scale_ffn = per_token[:, 2 * D : 3 * D]
    gate_ffn = per_token[:, 3 * D :]

    def lanes(columns):
        rows = columns.shape[0]
        return jnp.pad(columns, ((0, 0), (HD, LANES - HD - columns.shape[1]))).astype(bf16)

    slot_ids = jnp.arange(slot_count, dtype=jnp.int32)
    slot_live = (slot_ids % TXT)[:, None] < text_lengths[0][None, :]
    slot_fits = ((slot_ids // TXT)[:, None] == image_ids[None, :]) & slot_live
    three = lambda rows: jnp.ones((rows, 3), f32)
    query_lanes = lanes(select_all)
    key_lanes = lanes(jnp.concatenate([(select_all - 1.0) * OFF, three(seq_len)], 1))
    text_lanes = lanes(
        jnp.concatenate([jnp.where(slot_fits, 0.0, -OFF), three(slot_count)], 1)
    )
    block_first = jnp.arange(seq_len // BQ, dtype=jnp.int32) * BQ
    in_first = jnp.sum((block_first[:, None] >= image_ends[None, :]).astype(jnp.int32), 1)
    in_last = jnp.sum(((block_first + BQ - 1)[:, None] >= image_ends[None, :]).astype(jnp.int32), 1)
    pick = lambda values, at: jnp.sum(
        jnp.where(at[:, None] == image_ids[None, :], values[None, :], 0), 1
    )
    bounds = jnp.stack(
        [
            pick(image_starts, in_first) // BK,
            (pick(image_ends, in_last) + BK - 1) // BK,
            in_first,
            in_last + 1,
            (block_first // local_rows ^ turn) * (local_rows // BQ) + block_first % local_rows // BQ,
        ]
    ).astype(jnp.int32)

    quarter = HD // 4
    frequency = 10000.0 ** (-jnp.arange(quarter, dtype=f32) / quarter)
    angles = (positions.astype(f32)[:, None, :] * frequency[None, :, None]).reshape(-1, seq_len)
    lane_ids = jnp.arange(LANES, dtype=jnp.int32)
    source = (lane_ids % HD) // (2 * quarter) * quarter + lane_ids % quarter
    spread = (jnp.arange(2 * quarter)[:, None] == source[None, :]).astype(f32)
    sign = jnp.where(lane_ids % (2 * quarter) < quarter, -1.0, 1.0)
    turn_rows = (((0,), (0,)), ((), ()))
    cos = lax.dot_general(jnp.cos(angles), spread, turn_rows, precision=highest)
    sin = lax.dot_general(jnp.sin(angles), spread * sign[None, :], turn_rows, precision=highest)

    hidden_float = hidden_in.astype(f32)
    normed_one, back_norm_one = jax.vjp(modulated_norm, hidden_float, attention_gain, scale_attn)
    normed_one_low = normed_one.astype(bf16)
    tanh_ffn = jnp.tanh(gate_ffn)
    cotangent = out_cotangent.astype(f32)
    d_ffn_low = (cotangent * tanh_ffn).astype(bf16)

    widen = lambda w: jnp.pad(w, ((0, 0), (0, spare))) if spare else w
    narrow = lambda d: d[:, :local_width] if spare else d
    w_joint = jnp.concatenate([widen(w_query), widen(w_key), widen(w_value)], 1)
    w_text = jnp.concatenate([widen(w_text_key), widen(w_text_value)], 1)
    w_out_wide = jnp.pad(w_out, ((0, spare), (0, 0))) if spare else w_out
    text_joint = jnp.dot(text_states, w_text, preferred_element_type=f32)
    gate_mine = lax.dynamic_slice_in_dim(head_gates, shard_index * local_heads, local_heads, 0)
    gate_tanh = jnp.tanh(gate_mine)
    gates = jnp.pad(gate_tanh, (0, wide // HD - local_heads))

    def cast_dot(left, right, numbers):
        return lax.dot_general(left, right, numbers, preferred_element_type=f32).astype(bf16)

    plain = (((1,), (0,)), ((), ()))

    def feed(rows):
        gate_pre = jnp.dot(rows, w_gate, preferred_element_type=f32)
        up_pre = jnp.dot(rows, w_up, preferred_element_type=f32)
        sigmoid_gate = jax.nn.sigmoid(gate_pre)
        activated = gate_pre * sigmoid_gate
        return gate_pre, up_pre, sigmoid_gate, activated, (activated * up_pre).astype(bf16)

    def feed_back(d_rows, gate_pre, up_pre, sigmoid_gate, activated, inner_low):
        d_inner = lax.dot_general(d_rows, w_down, contract_cols, preferred_element_type=f32)
        d_gate_low = (
            d_inner * up_pre * sigmoid_gate * (1.0 + gate_pre * (1.0 - sigmoid_gate))
        ).astype(bf16)
        d_up_low = (d_inner * activated).astype(bf16)
        d_normed = (
            lax.dot_general(d_gate_low, w_gate, contract_cols, preferred_element_type=f32)
            + lax.dot_general(d_up_low, w_up, contract_cols, preferred_element_type=f32)
        ).astype(bf16)
        return d_gate_low, d_up_low, d_normed

    def grad_of(lefts, rights):
        return sum(
            lax.dot_general(left, right, contract_rows, preferred_element_type=f32)
            for left, right in zip(lefts, rights)
        ).astype(bf16)

    def sum_packs(joined):
        return lax.psum_scatter(joined, "dp", scatter_dimension=0, tiled=True)

    if halves:
        across = swapped(normed_one_low, "mp", 2)
        near, far = near_rows(normed_one_low), far_rows(normed_one_low, across)
        rows_attn = jnp.concatenate([near, far], 0)
    else:
        rows_attn = lax.all_gather(normed_one_low, "mp", axis=0, tiled=True)
    joint = jnp.dot(rows_attn, w_joint, preferred_element_type=f32)
    joint, d_ffn_low = lax.optimization_barrier((joint, d_ffn_low))
    if halves:
        across_d = swapped(d_ffn_low, "mp", 2)
    else:
        d_rows = (lax.all_gather(d_ffn_low, "mp", axis=0, tiled=True),)
    mixed_low, *saved = attend(
        bounds, gates, joint, text_joint, cos, sin, query_lanes, key_lanes, text_lanes
    )
    if halves:
        mixed_low, across_d = lax.optimization_barrier((mixed_low, across_d))
        d_rows = (near_rows(d_ffn_low), far_rows(d_ffn_low, across_d))

    def project(rows):
        return cast_dot(rows, w_out_wide, plain)

    half = seq_len // 2
    if halves:
        far_out = to_across(project(mixed_low[half:]))
        attention_out = own_sum(project(mixed_low[:half]), swapped(far_out, "mp", 2))
    else:
        attention_out = lax.psum_scatter(
            project(mixed_low), "mp", scatter_dimension=0, tiled=True
        ).astype(f32)
    tanh_attn = jnp.tanh(gate_attn)
    after_attn = hidden_float + tanh_attn * attention_out
    normed_two, back_norm_two = jax.vjp(modulated_norm, after_attn, feedforward_gain, scale_ffn)
    normed_two_low = normed_two.astype(bf16)
    if halves:
        across = swapped(normed_two_low, "mp", 2)
        near = near_rows(normed_two_low)
        fed_near = feed(near)
        back_near = feed_back(d_rows[0], *fed_near)
        ffn_near = cast_dot(fed_near[-1], w_down, plain)
        across = after(across, back_near[-1], ffn_near)
        far = far_rows(normed_two_low, across)
        fed_far = feed(far)
        back_far = feed_back(d_rows[1], *fed_far)
        rows_ffn, inner, d_gate, d_up = (
            (near, far),
            (fed_near[-1], fed_far[-1]),
            (back_near[0], back_far[0]),
            (back_near[1], back_far[1]),
        )
        other = swapped(to_across(back_far[-1]), "mp", 2)
        ffn_far = cast_dot(after(fed_far[-1], back_far[-1]), w_down, plain)
    else:
        rows_ffn = (lax.all_gather(normed_two_low, "mp", axis=0, tiled=True),)
        fed = feed(rows_ffn[0])
        back = feed_back(d_rows[0], *fed)
        inner, d_gate, d_up = (fed[-1],), (back[0],), (back[1],)
        d_normed_two = lax.psum_scatter(back[-1], "mp", scatter_dimension=0, tiled=True).astype(f32)
        ffn_out = lax.psum_scatter(
            cast_dot(fed[-1], w_down, plain), "mp", scatter_dimension=0, tiled=True
        ).astype(f32)
    joined_ffn = jnp.concatenate(
        [grad_of(rows_ffn, d_gate), grad_of(rows_ffn, d_up), grad_of(d_rows, inner)], 1
    )
    if halves:
        other, joined_ffn, ffn_far = lax.optimization_barrier((other, joined_ffn, ffn_far))
        d_normed_two = own_sum(back_near[-1], other)
    out_ffn = sum_packs(joined_ffn)

    d_after_norm, grad_ffn_gain, d_scale_ffn = back_norm_two(d_normed_two)
    d_after = cotangent + d_after_norm
    d_attn_low = (d_after * tanh_attn).astype(bf16)
    d_gate_attn = d_after * attention_out * (1.0 - tanh_attn * tanh_attn)
    if halves:
        across = swapped(d_attn_low, "mp", 2)
        d_attn_all = jnp.concatenate([near_rows(d_attn_low), far_rows(d_attn_low, across)], 0)
    else:
        d_attn_all = lax.all_gather(d_attn_low, "mp", axis=0, tiled=True)
    d_mixed = lax.dot_general(d_attn_all, w_out_wide, contract_cols, preferred_element_type=f32)
    if halves:
        other = swapped(to_across(after(ffn_far, d_mixed)), "mp", 2)
    d_query, d_key, d_value, d_text_key, d_text_value, d_heads = attend_back(
        bounds, gates, d_mixed, saved, joint, text_joint, cos, sin
    )
    if halves:
        d_text_key, other = lax.optimization_barrier((d_text_key, other))
        ffn_out = own_sum(ffn_near, other)
    block_out = (after_attn + tanh_ffn * ffn_out).astype(bf16)
    d_gate_ffn = cotangent * ffn_out * (1.0 - tanh_ffn * tanh_ffn)
    grad_heads = jnp.sum(d_heads, 1).reshape(wide // HD, HD).sum(1)[:local_heads]
    grad_heads = grad_heads * (1.0 - gate_tanh * gate_tanh)
    d_text_low = jnp.concatenate([narrow(d_text_key), narrow(d_text_value)], 1)
    joined_text = grad_of((text_states,), (d_text_low,))
    joined_text, out_ffn = lax.optimization_barrier((joined_text, out_ffn))
    out_text = sum_packs(joined_text)
    d_joint_low = after(jnp.concatenate([d_query, d_key, d_value], 1), joined_text)
    d_rows_one = lambda d: cast_dot(d, w_joint, contract_cols)
    if halves:
        other = swapped(to_across(d_rows_one(d_joint_low[half:])), "mp", 2)
        near_one = d_rows_one(d_joint_low[:half])
    else:
        d_normed_one = lax.psum_scatter(
            d_rows_one(d_joint_low), "mp", scatter_dimension=0, tiled=True
        ).astype(f32)
    joined_attn = jnp.concatenate(
        [
            grad_of((rows_attn,), (narrow(d_query),)),
            grad_of((rows_attn,), (narrow(d_key),)),
            grad_of((rows_attn,), (narrow(d_value),)),
            grad_of((d_attn_all,), (narrow(mixed_low),)),
        ],
        1,
    ) if spare else jnp.concatenate(
        [grad_of((rows_attn,), (d_joint_low,)), grad_of((d_attn_all,), (mixed_low,))], 1
    )
    if halves:
        other, joined_attn = lax.optimization_barrier((other, joined_attn))
        d_normed_one = own_sum(near_one, other)
    out_attn = sum_packs(joined_attn)
    out_attn, out_text, out_ffn = (out.astype(f32) for out in (out_attn, out_text, out_ffn))

    d_hidden_norm, grad_attn_gain, d_scale_attn = back_norm_one(d_normed_one)
    input_grad = (d_after + d_hidden_norm).astype(bf16)
    d_per_token = jnp.concatenate([d_scale_attn, d_gate_attn, d_scale_ffn, d_gate_ffn], 1)
    mod_partial = lax.dot_general(select_mine, d_per_token, contract_rows, precision=highest)
    modulation_grad = sum_over(mod_partial, ("mp",))[None]
    heads_full = lax.dynamic_update_slice(
        jnp.zeros((H,), f32), grad_heads, (shard_index * local_heads,)
    )
    small = jnp.concatenate([grad_attn_gain, grad_ffn_gain, heads_full])
    small = sum_over(small, ("mp", "dp"))
    return (
        block_out,
        input_grad,
        modulation_grad,
        out_attn[:, 0:local_width],
        out_attn[:, local_width : 2 * local_width],
        out_attn[:, 2 * local_width : 3 * local_width],
        out_attn[:, 3 * local_width :].T,
        out_text[:, 0:local_width],
        out_text[:, local_width:],
        out_ffn[:, 0:hidden],
        out_ffn[:, hidden : 2 * hidden],
        out_ffn[:, 2 * hidden :].T,
        small[0:D],
        small[D : 2 * D],
        small[2 * D :],
    )


def solution(mesh):
    placed = (
        P(("dp", "mp"), None),
        P("dp", None),
        P("dp", None, None),
        P("dp", None),
        P("dp", None),
        P(None, "dp"),
        P(None, "mp"),
        P(None, "mp"),
        P(None, "mp"),
        P("mp", None),
        P(None, "mp"),
        P(None, "mp"),
        P(None, "mp"),
        P(None, "mp"),
        P("mp", None),
        P(),
        P(),
        P(),
        P(("dp", "mp"), None),
    )
    return jax.shard_map(
        on_device,
        mesh=mesh,
        in_specs=placed,
        out_specs=(
            P(("dp", "mp"), None),
            P(("dp", "mp"), None),
            P("dp", None, None),
            P("dp", "mp"),
            P("dp", "mp"),
            P("dp", "mp"),
            P("mp", "dp"),
            P("dp", "mp"),
            P("dp", "mp"),
            P("dp", "mp"),
            P("dp", "mp"),
            P("mp", "dp"),
            P(),
            P(),
            P(),
        ),
        check_vma=False,
    )
```
